32 devices in a mesh: dp: 8 (over y, x, core), seq: 4 (over z).
Axes of the slice: x: 2, y: 2, z: 4, core: 2. Of those that a mesh axis runs over, the one named last changes fastest.
Arguments:
- hidden_in: bfloat16 [8192, 1536], P(('dp', 'seq')), may hold values from -6 to 6
- item_ids: int32 [8192], P(('dp', 'seq')), may hold values from 0 to 15, as said below
- positions: int32 [8192], P(('dp', 'seq')), may hold values from 0 to 1023, as said below
- attn_gain: float32 [1536], P('dp'), may hold values from 0.1 to 1.9
- w_query: float32 [1536, 1536], P('dp'), may hold values from -0.15625 to 0.15625
- key_weight: float32 [1536, 768], P('dp'), may hold values from -0.15625 to 0.15625
- value_weight: float32 [1536, 768], P('dp'), may hold values from -0.15625 to 0.15625
- w_output: float32 [1536, 1536], P('dp'), may hold values from -0.625 to 0.625
- ffn_gain: float32 [1536], P('dp'), may hold values from 0.1 to 1.9
- w_gate: float32 [1536, 4096], P('dp'), may hold values from -0.15625 to 0.15625
- w_up: float32 [1536, 4096], P('dp'), may hold values from -0.15625 to 0.15625
- w_down: float32 [4096, 1536], P('dp'), may hold values from -0.09375 to 0.09375
- out_grad: bfloat16 [8192, 1536], P(('dp', 'seq')), may hold values from -6 to 6
Outputs:
- layer_out: bfloat16 [8192, 1536], P(('dp', 'seq'))
- input_grad: bfloat16 [8192, 1536], P(('dp', 'seq'))
- grad_attn_gain: float32 [1536], P('dp')
- grad_query: float32 [1536, 1536], P('dp')
- grad_key: float32 [1536, 768], P('dp')
- grad_value: float32 [1536, 768], P('dp')
- grad_output: float32 [1536, 1536], P('dp')
- grad_ffn_gain: float32 [1536], P('dp')
- grad_gate: float32 [1536, 4096], P('dp')
- grad_up: float32 [1536, 4096], P('dp')
- grad_down: float32 [4096, 1536], P('dp')
The draws below stay inside these ranges and needn't reach their ends.
Inputs may be any that keep to these rules, and one draw needn't show every extreme that they name: `item_ids`: ids never fall along the packed order, an item holds at most 1024 tokens and never spans a multiple of 1024 in the packed order. `positions`: a token's offset from the first token of its item.
All inputs are finite; a program needn't handle non-finite values.
Results may differ from the reference program's by a relative error of at most 0.014.
The reference program's roundings to bfloat16 on the way count: a program that leaves them out, or rounds other values in their place, can miss the bound.
Values may be sent and summed in bfloat16 or wider, within the bound.
A program may use at most 320 MiB of HBM per device.

```python
import jax
import jax.numpy as jnp
from jax import lax

MODEL_WIDTH = 1536
QUERY_HEADS = 16
KEY_VALUE_HEADS = 8
HEAD_SIZE = 96
FF = 4096
SLIDE_SPAN = 512
ITEM_MAX = 1024
TOKENS = 8192


def item_layout(key):
    blocks = TOKENS // ITEM_MAX
    key_cut, key_whole = jax.random.split(jax.random.fold_in(key, 11))
    cut_points = jax.random.randint(key_cut, (blocks,), ITEM_MAX // 8, ITEM_MAX - ITEM_MAX // 8, dtype=jnp.int32)
    whole_block = jax.random.randint(key_whole, (), 0, blocks - 1, dtype=jnp.int32)
    cut_points = jnp.where(jnp.arange(blocks, dtype=jnp.int32) == whole_block, ITEM_MAX, cut_points)
    offsets = jnp.arange(ITEM_MAX, dtype=jnp.int32)
    second_item = (offsets[None, :] >= cut_points[:, None]).astype(jnp.int32)
    item_of = 2 * jnp.arange(blocks, dtype=jnp.int32)[:, None] + second_item
    token_positions = offsets[None, :] - second_item * cut_points[:, None]
    return (item_of.reshape(-1), token_positions.reshape(-1))


def draw_item_ids(key, part):
    return item_layout(key)[0]


def draw_positions(key, part):
    return item_layout(key)[1]


def levels(stream_key, extent, cuts, least, largest):
    loudness, own = 1.0, jax.random.fold_in(stream_key, 6)
    for position, shards_of in cuts:
        draws = jnp.exp(jax.random.uniform(jax.random.fold_in(own, position), (shards_of,), jnp.float32, least / len(cuts), largest / len(cuts)))
        loudness = loudness * jnp.repeat(draws, extent[position] // shards_of).reshape([-1 if axis == position else 1 for axis in range(len(extent))])
    return loudness


def noise(own_key, dims, deviation, limit, cuts=(), kind=jnp.bfloat16):
    drawn = jax.random.normal(own_key, dims, jnp.float32) * deviation
    if len(cuts) > 0:
        drawn = levels(own_key, dims, cuts, -0.22, 0.18) * drawn
    return jnp.clip(drawn, min=-limit, max=limit).astype(kind)


def setup_inputs(seed: int = 0) -> dict:
    streams_of = jax.random.split(jax.random.key(seed), 14)
    hidden_in = noise(streams_of[0], (TOKENS, MODEL_WIDTH), 1.0, 6.0, ((0, 32),))
    item_ids = draw_item_ids(jax.random.fold_in(streams_of[13], 71), 0)
    positions = draw_positions(jax.random.fold_in(streams_of[13], 71), 0)
    attn_gain = jnp.clip(1.0 + 0.18 * jax.random.normal(streams_of[3], (MODEL_WIDTH,), jnp.float32), 0.1, 1.9)
    w_query = noise(streams_of[4], (MODEL_WIDTH, QUERY_HEADS * HEAD_SIZE), MODEL_WIDTH ** -0.5, 0.15625, ((0, 8),), jnp.float32)
    key_weight = noise(streams_of[5], (MODEL_WIDTH, KEY_VALUE_HEADS * HEAD_SIZE), MODEL_WIDTH ** -0.5, 0.15625, ((0, 8),), jnp.float32)
    value_weight = noise(streams_of[6], (MODEL_WIDTH, KEY_VALUE_HEADS * HEAD_SIZE), MODEL_WIDTH ** -0.5, 0.15625, ((0, 8),), jnp.float32)
    w_output = noise(streams_of[7], (QUERY_HEADS * HEAD_SIZE, MODEL_WIDTH), (QUERY_HEADS * HEAD_SIZE // 16) ** -0.5, 0.625, ((0, 8),), jnp.float32)
    ffn_gain = jnp.clip(1.0 + 0.18 * jax.random.normal(streams_of[8], (MODEL_WIDTH,), jnp.float32), 0.1, 1.9)
    w_gate = noise(streams_of[9], (MODEL_WIDTH, FF), MODEL_WIDTH ** -0.5, 0.15625, ((0, 8),), jnp.float32)
    w_up = noise(streams_of[10], (MODEL_WIDTH, FF), MODEL_WIDTH ** -0.5, 0.15625, ((0, 8),), jnp.float32)
    w_down = noise(streams_of[11], (FF, MODEL_WIDTH), FF ** -0.5, 0.09375, ((0, 8),), jnp.float32)
    out_grad = noise(streams_of[12], (TOKENS, MODEL_WIDTH), 1.0, 6.0, ((0, 32),))
    return {"hidden_in": hidden_in, "item_ids": item_ids, "positions": positions, "attn_gain": attn_gain, "w_query": w_query, "key_weight": key_weight, "value_weight": value_weight, "w_output": w_output, "ffn_gain": ffn_gain, "w_gate": w_gate, "w_up": w_up, "w_down": w_down, "out_grad": out_grad}


@jax.custom_vjp
def low(v):
    return lax.optimization_barrier(v.astype(jnp.bfloat16)).astype(jnp.float32)

@jax.custom_vjp
def low_back(v):
    return v

def low_keep(v):
    return (low(v), None)

def low_pass(kept, grad):
    return (grad,)

def back_keep(v):
    return (v, None)

def back_low(kept, grad):
    return (low(grad),)
low.defvjp(low_keep, low_pass)
low_back.defvjp(back_keep, back_low)
eps_norm = 1e-05
rope_base = 100000.0
masked_fill = -1e+30

def apply_rotary(value_rows, token_positions, direction):
    half_dim = value_rows.shape[-1] // 2
    frequency = rope_base ** (-(jnp.arange(half_dim, dtype=jnp.float32) * 2.0 / value_rows.shape[-1]))
    angles = token_positions.astype(jnp.float32)[:, None] * frequency[None, :]
    cosine = jnp.cos(angles)[:, None, :]
    sine_part = direction * jnp.sin(angles)[:, None, :]
    front_half = value_rows[..., :half_dim]
    back_half = value_rows[..., half_dim:]
    return jnp.concatenate([front_half * cosine - back_half * sine_part, back_half * cosine + front_half * sine_part], -1)

def product_result(left, right):
    return jnp.dot(left, right, precision=lax.Precision.HIGHEST)

def attend(query_rows, key_rows, value_rows, item_of):
    token_total = query_rows.shape[0]
    query_group_count = QUERY_HEADS // KEY_VALUE_HEADS
    score_scale = HEAD_SIZE ** (-0.5)
    key_rows_padded = jnp.concatenate([jnp.zeros((SLIDE_SPAN, KEY_VALUE_HEADS, HEAD_SIZE), key_rows.dtype), key_rows], 0)
    value_rows_padded = jnp.concatenate([jnp.zeros((SLIDE_SPAN, KEY_VALUE_HEADS, HEAD_SIZE), value_rows.dtype), value_rows], 0)
    padded_items = jnp.concatenate([jnp.full((SLIDE_SPAN,), -1, jnp.int32), item_of.astype(jnp.int32)], 0)
    grouped_queries = query_rows.reshape(token_total, KEY_VALUE_HEADS, query_group_count, HEAD_SIZE)
    query_index = jnp.arange(SLIDE_SPAN, dtype=jnp.int32)[:, None]
    key_index = jnp.arange(2 * SLIDE_SPAN, dtype=jnp.int32)[None, :]
    distance = query_index + SLIDE_SPAN - key_index
    within = (distance >= 0) & (distance <= SLIDE_SPAN)

    def one_block(index):
        start = (index * SLIDE_SPAN).astype(jnp.int32)
        query_block = lax.dynamic_slice_in_dim(grouped_queries, start, SLIDE_SPAN, 0)
        key_block = lax.dynamic_slice_in_dim(key_rows_padded, start, 2 * SLIDE_SPAN, 0)
        value_block = lax.dynamic_slice_in_dim(value_rows_padded, start, 2 * SLIDE_SPAN, 0)
        query_items = lax.dynamic_slice_in_dim(item_of.astype(jnp.int32), start, SLIDE_SPAN, 0)
        key_items = lax.dynamic_slice_in_dim(padded_items, start, 2 * SLIDE_SPAN, 0)
        allowed = within & (query_items[:, None] == key_items[None, :])
        raw_scores = jnp.einsum('tgrd,kgd->grtk', query_block, key_block, precision=lax.Precision.HIGHEST) * score_scale
        raw_scores = low_back(raw_scores)
        raw_scores = jnp.where(allowed[None, None], raw_scores, masked_fill)
        probs = jax.nn.softmax(raw_scores, axis=-1)
        weighted = jnp.einsum('grtk,kgd->tgrd', low(probs), value_block, precision=lax.Precision.HIGHEST)
        return weighted.reshape(SLIDE_SPAN, QUERY_HEADS * HEAD_SIZE)
    blocks = token_total // SLIDE_SPAN
    result = lax.map(jax.checkpoint(one_block), jnp.arange(blocks, dtype=jnp.int32))
    return result.reshape(token_total, QUERY_HEADS * HEAD_SIZE)

def block_forward(inputs, item_of, token_positions, attn_gain, w_query, key_weight, value_weight, w_output, ffn_gain, w_gate, w_up, w_down):
    token_total = inputs.shape[0]
    normed_one = inputs * lax.rsqrt(lax.optimization_barrier(jnp.mean(inputs * inputs, -1, keepdims=True)) + eps_norm)
    scaled_first_norm = low(normed_one * low(attn_gain))
    query_rows = low(apply_rotary(low_back(product_result(scaled_first_norm, low(w_query))).reshape(token_total, QUERY_HEADS, HEAD_SIZE), token_positions, 1.0))
    key_rows = low(apply_rotary(low_back(product_result(scaled_first_norm, low(key_weight))).reshape(token_total, KEY_VALUE_HEADS, HEAD_SIZE), token_positions, 1.0))
    value_rows = low(low_back(product_result(scaled_first_norm, low(value_weight)))).reshape(token_total, KEY_VALUE_HEADS, HEAD_SIZE)
    attended = low(low_back(attend(query_rows, key_rows, value_rows, item_of)))
    middle = inputs + low_back(product_result(attended, low(w_output)))
    normed_two = middle * lax.rsqrt(lax.optimization_barrier(jnp.mean(middle * middle, -1, keepdims=True)) + eps_norm)
    gained_two = low(normed_two * low(ffn_gain))
    gate_pre = low_back(product_result(gained_two, low(w_gate)))
    up_pre = low_back(product_result(gained_two, low(w_up)))
    hidden = low(jax.nn.silu(gate_pre) * up_pre)
    return middle + product_result(hidden, low(w_down))

def reference(hidden_in, item_ids, positions, attn_gain, w_query, key_weight, value_weight, w_output, ffn_gain, w_gate, w_up, w_down, out_grad):
    blocks = TOKENS // ITEM_MAX
    weights = (attn_gain, w_query, key_weight, value_weight, w_output, ffn_gain, w_gate, w_up, w_down)
    inputs = hidden_in.astype(jnp.float32).reshape(blocks, ITEM_MAX, MODEL_WIDTH)
    cotangent = out_grad.astype(jnp.float32).reshape(blocks, ITEM_MAX, MODEL_WIDTH)
    item_blocks = item_ids.reshape(blocks, ITEM_MAX)
    place_blocks = positions.reshape(blocks, ITEM_MAX)

    def one_item_block(summed, packed):
        block_in, block_items, block_places, block_cot = packed

        def forward(x_in, params):
            return block_forward(x_in, block_items, block_places, *params)
        result, pullback = jax.vjp(forward, block_in, weights)
        grad_in, grad_params = pullback(block_cot)
        summed = jax.tree.map(jnp.add, summed, grad_params)
        return (summed, (result.astype(jnp.bfloat16), grad_in.astype(jnp.bfloat16)))
    zero_filled = jax.tree.map(jnp.zeros_like, weights)
    summed, (results, grads) = lax.scan(one_item_block, zero_filled, (inputs, item_blocks, place_blocks, cotangent))
    return (results.reshape(TOKENS, MODEL_WIDTH), grads.reshape(TOKENS, MODEL_WIDTH), summed[0], summed[1], summed[2], summed[3], summed[4], summed[5], summed[6], summed[7], summed[8])
```

```python
import jax
import jax.numpy as jnp
from jax import lax
from jax.sharding import PartitionSpec as P

QUERY_HEADS = 16
KEY_VALUE_HEADS = 8
HEAD_SIZE = 96
SLIDE_SPAN = 512


eps_norm = 1e-05
rope_base = 100000.0
masked_fill = -1e30


def passed_along(block, axis, distance):
    devices = range(lax.axis_size(axis))
    route = [(i - distance, i) for i in devices if i - distance in devices]
    return lax.ppermute(block, axis, route)


def apply_rotary(value_rows, token_positions, direction):
    half_dim = value_rows.shape[-1] // 2
    frequency = rope_base ** (
        -(jnp.arange(half_dim, dtype=jnp.float32) * 2.0 / value_rows.shape[-1])
    )
    angles = token_positions.astype(jnp.float32)[:, None] * frequency[None, :]
    cosine = jnp.cos(angles)[:, None, :]
    sine_part = direction * jnp.sin(angles)[:, None, :]
    front_half = value_rows[..., :half_dim]
    back_half = value_rows[..., half_dim:]
    return jnp.concatenate(
        [front_half * cosine - back_half * sine_part, back_half * cosine + front_half * sine_part],
        -1,
    )


def matrix_product(left, right):
    return jnp.dot(left, right, preferred_element_type=jnp.float32)


def contract_rows(left, right):
    return jnp.einsum("ta,tb->ab", left, right, preferred_element_type=jnp.float32)


def product_transposed(left, right):
    return jnp.einsum("ta,ba->tb", left, right, preferred_element_type=jnp.float32)


def norm_back(grad_normed, normed, inverse):
    return inverse * (grad_normed - normed * jnp.mean(grad_normed * normed, -1, keepdims=True))


def per_device(
    hidden_in,
    item_ids,
    positions,
    attn_gain,
    w_query,
    key_weight,
    value_weight,
    w_output,
    ffn_gain,
    w_gate,
    w_up,
    w_down,
    out_grad,
):
    token_count = hidden_in.shape[0]
    query_group_count = QUERY_HEADS // KEY_VALUE_HEADS
    score_scale = HEAD_SIZE ** (-0.5)
    halo_rows = min(token_count, SLIDE_SPAN)
    halo_steps = max(1, SLIDE_SPAN // token_count)
    reduced_element_type = jnp.bfloat16
    gain_one, query_w, key_matrix, value_w, output_matrix = (
        lax.all_gather(attn_gain.astype(reduced_element_type), "dp", axis=0, tiled=True),
        lax.all_gather(w_query.astype(reduced_element_type), "dp", axis=0, tiled=True),
        lax.all_gather(key_weight.astype(reduced_element_type), "dp", axis=0, tiled=True),
        lax.all_gather(value_weight.astype(reduced_element_type), "dp", axis=0, tiled=True),
        lax.all_gather(w_output.astype(reduced_element_type), "dp", axis=0, tiled=True),
    )
    gain_two, gate_w, up_w, down_w = (
        lax.all_gather(ffn_gain.astype(reduced_element_type), "dp", axis=0, tiled=True),
        lax.all_gather(w_gate.astype(reduced_element_type), "dp", axis=0, tiled=True),
        lax.all_gather(w_up.astype(reduced_element_type), "dp", axis=0, tiled=True),
        lax.all_gather(w_down.astype(reduced_element_type), "dp", axis=0, tiled=True),
    )
    inputs = hidden_in.astype(jnp.float32)
    inverse_one = lax.rsqrt(jnp.mean(inputs * inputs, -1, keepdims=True) + eps_norm)
    normed_one = inputs * inverse_one
    gain_one_full = gain_one.astype(jnp.float32)
    scaled_first_norm = (normed_one * gain_one_full).astype(reduced_element_type)
    query_unrotated = matrix_product(scaled_first_norm, query_w).reshape(
        token_count, QUERY_HEADS, HEAD_SIZE
    )
    key_unrotated = matrix_product(scaled_first_norm, key_matrix).reshape(
        token_count, KEY_VALUE_HEADS, HEAD_SIZE
    )
    value_projected = matrix_product(scaled_first_norm, value_w)
    query_rot = (
        apply_rotary(query_unrotated, positions, 1.0)
        .astype(reduced_element_type)
        .reshape(token_count, KEY_VALUE_HEADS, query_group_count, HEAD_SIZE)
    )
    key_rot = apply_rotary(key_unrotated, positions, 1.0).astype(reduced_element_type)
    value_reduced = value_projected.astype(reduced_element_type).reshape(
        token_count, KEY_VALUE_HEADS, HEAD_SIZE
    )
    item_marks = item_ids + 1
    key_parts = []
    value_parts = []
    mark_parts = []
    for offset in range(halo_steps, 0, -1):
        incoming = passed_along((key_rot, value_reduced, item_marks), ("dp", "seq"), offset)
        key_parts.append(incoming[0])
        value_parts.append(incoming[1])
        mark_parts.append(incoming[2])
    all_keys = jnp.concatenate(key_parts + [key_rot], 0)
    all_values = jnp.concatenate(value_parts + [value_reduced], 0)
    all_marks = jnp.concatenate(mark_parts + [item_marks], 0)
    query_index = jnp.arange(token_count, dtype=jnp.int32)[:, None]
    key_index = jnp.arange(SLIDE_SPAN + token_count, dtype=jnp.int32)[None, :]
    distance = query_index + SLIDE_SPAN - key_index
    allowed = (
        (distance >= 0) & (distance <= SLIDE_SPAN) & (item_marks[:, None] == all_marks[None, :])
    )

    def masked_scores():
        raw_scores = (
            jnp.einsum("tgrd,kgd->grtk", query_rot, all_keys, preferred_element_type=jnp.float32)
            * score_scale
        )
        return jnp.where(allowed[None, None], raw_scores, masked_fill)

    scores = masked_scores()
    row_max = jnp.max(scores, -1, keepdims=True)
    log_total = row_max + jnp.log(jnp.sum(jnp.exp(scores - row_max), -1, keepdims=True))
    probs_low = jnp.exp(scores - log_total).astype(reduced_element_type)
    attended_low = (
        jnp.einsum("grtk,kgd->tgrd", probs_low, all_values, preferred_element_type=jnp.float32)
        .reshape(token_count, QUERY_HEADS * HEAD_SIZE)
        .astype(reduced_element_type)
    )
    middle = inputs + matrix_product(attended_low, output_matrix)
    inverse_two = lax.rsqrt(jnp.mean(middle * middle, -1, keepdims=True) + eps_norm)
    normed_two = middle * inverse_two
    gain_two_full = gain_two.astype(jnp.float32)
    gained_two = (normed_two * gain_two_full).astype(reduced_element_type)
    gate_pre = matrix_product(gained_two, gate_w)
    up_pre = matrix_product(gained_two, up_w)
    gate_sig = jax.nn.sigmoid(gate_pre)
    gate_act = gate_pre * gate_sig
    hidden_low = (gate_act * up_pre).astype(reduced_element_type)
    layer_out = (middle + matrix_product(hidden_low, down_w)).astype(reduced_element_type)
    grad_down_w = contract_rows(hidden_low, out_grad)
    grad_hidden = product_transposed(out_grad, down_w)
    grad_gate_low = (grad_hidden * up_pre * gate_sig * (1.0 + gate_pre * (1.0 - gate_sig))).astype(
        reduced_element_type
    )
    grad_up_low = (grad_hidden * gate_act).astype(reduced_element_type)
    grad_gate_w = contract_rows(gained_two, grad_gate_low)
    grad_up_w = contract_rows(gained_two, grad_up_low)
    grad_gained_two = product_transposed(grad_gate_low, gate_w) + product_transposed(
        grad_up_low, up_w
    )
    grad_gain_two = jnp.sum(grad_gained_two * normed_two, 0)
    grad_middle = out_grad.astype(jnp.float32) + norm_back(
        grad_gained_two * gain_two_full, normed_two, inverse_two
    )
    ffn_shards = (
        lax.psum_scatter(grad_gain_two, "dp", scatter_dimension=0, tiled=True),
        lax.psum_scatter(grad_gate_w, "dp", scatter_dimension=0, tiled=True),
        lax.psum_scatter(grad_up_w, "dp", scatter_dimension=0, tiled=True),
        lax.psum_scatter(grad_down_w, "dp", scatter_dimension=0, tiled=True),
    )
    branch_gradient = grad_middle.astype(reduced_element_type)
    grad_output_w = contract_rows(attended_low, branch_gradient)
    grad_attended = (
        product_transposed(branch_gradient, output_matrix)
        .astype(reduced_element_type)
        .reshape(token_count, KEY_VALUE_HEADS, query_group_count, HEAD_SIZE)
    )
    scores_again = masked_scores()
    probs_again = jnp.exp(scores_again - log_total)
    grad_probs = jnp.einsum(
        "tgrd,kgd->grtk", grad_attended, all_values, preferred_element_type=jnp.float32
    )
    row_dot = jnp.sum(probs_again * grad_probs, -1, keepdims=True)
    grad_scores = (probs_again * (grad_probs - row_dot)).astype(reduced_element_type)
    grad_query = (
        jnp.einsum(
            "grtk,kgd->tgrd", grad_scores, all_keys, preferred_element_type=jnp.float32
        ).reshape(token_count, QUERY_HEADS, HEAD_SIZE)
        * score_scale
    )
    grad_keys = (
        jnp.einsum("grtk,tgrd->kgd", grad_scores, query_rot, preferred_element_type=jnp.float32)
        * score_scale
    )
    grad_values = jnp.einsum(
        "grtk,tgrd->kgd", probs_low, grad_attended, preferred_element_type=jnp.float32
    )
    key_neighbourhood = grad_keys[SLIDE_SPAN:]
    value_neighbourhood = grad_values[SLIDE_SPAN:]
    for offset in range(1, halo_steps + 1):
        first_row = (halo_steps - offset) * halo_rows
        returned = passed_along(
            (
                grad_keys[first_row : first_row + halo_rows],
                grad_values[first_row : first_row + halo_rows],
            ),
            ("dp", "seq"),
            -offset,
        )
        key_neighbourhood = key_neighbourhood.at[token_count - halo_rows :].add(returned[0])
        value_neighbourhood = value_neighbourhood.at[token_count - halo_rows :].add(returned[1])
    grad_query_low = (
        apply_rotary(grad_query, positions, -1.0)
        .astype(reduced_element_type)
        .reshape(token_count, QUERY_HEADS * HEAD_SIZE)
    )
    key_gradient_reduced = (
        apply_rotary(key_neighbourhood, positions, -1.0)
        .astype(reduced_element_type)
        .reshape(token_count, KEY_VALUE_HEADS * HEAD_SIZE)
    )
    value_gradient_reduced = value_neighbourhood.astype(reduced_element_type).reshape(
        token_count, KEY_VALUE_HEADS * HEAD_SIZE
    )
    grad_query_w = contract_rows(scaled_first_norm, grad_query_low)
    grad_key_w = contract_rows(scaled_first_norm, key_gradient_reduced)
    grad_value_w = contract_rows(scaled_first_norm, value_gradient_reduced)
    grad_gained_one = (
        product_transposed(grad_query_low, query_w)
        + product_transposed(key_gradient_reduced, key_matrix)
        + product_transposed(value_gradient_reduced, value_w)
    )
    grad_gain_one = jnp.sum(grad_gained_one * normed_one, 0)
    input_grad = (
        grad_middle + norm_back(grad_gained_one * gain_one_full, normed_one, inverse_one)
    ).astype(reduced_element_type)
    attn_shards = (
        lax.psum_scatter(grad_gain_one, "dp", scatter_dimension=0, tiled=True),
        lax.psum_scatter(grad_query_w, "dp", scatter_dimension=0, tiled=True),
        lax.psum_scatter(grad_key_w, "dp", scatter_dimension=0, tiled=True),
        lax.psum_scatter(grad_value_w, "dp", scatter_dimension=0, tiled=True),
        lax.psum_scatter(grad_output_w, "dp", scatter_dimension=0, tiled=True),
    )
    summed = lax.psum(
        (
            attn_shards[0],
            attn_shards[1],
            attn_shards[2],
            attn_shards[3],
            attn_shards[4],
            ffn_shards[0],
            ffn_shards[1],
            ffn_shards[2],
            ffn_shards[3],
        ),
        "seq",
    )
    return (
        layer_out,
        input_grad,
        summed[0],
        summed[1],
        summed[2],
        summed[3],
        summed[4],
        summed[5],
        summed[6],
        summed[7],
        summed[8],
    )


def swapped(block, axis, bit):
    route = [(i, i ^ bit) for i in range(lax.axis_size(axis))]
    return lax.ppermute(block, axis, route)


def chosen(bit, first, second):
    return jnp.where(bit == 0, first, second)


def in_order(bit, own, other):
    return chosen(bit, jnp.stack([own, other]), jnp.stack([other, own]))


def mesh_bits():
    block, part = lax.axis_index("dp"), lax.axis_index("seq")
    return block // 4, (block // 2) % 2, block % 2, part // 2, part % 2


CORE, ALONG_X, ALONG_Y = ("dp", 1), ("dp", 2), ("dp", 4)
Z_NEAR, Z_FAR = ("seq", 1), ("seq", 2)


def gather_plane(first, second, y, x):
    first_x = in_order(x, first, swapped(first, *ALONG_X))
    second_y = in_order(y, second, swapped(second, *ALONG_Y))
    first_all = in_order(y, first_x, swapped(first_x, *ALONG_Y))
    second_other = swapped(second_y, *ALONG_X)
    second_all = chosen(
        x,
        jnp.stack([second_y, second_other], 1),
        jnp.stack([second_other, second_y], 1),
    )
    return first_all, second_all


def picked(blocks, index, axis=0):
    return lax.dynamic_index_in_dim(blocks, index, axis, keepdims=False)


def wide(v):
    return v.astype(jnp.float32)


def low(v):
    return v.astype(jnp.bfloat16)


def reduce_plane(first, second, y, x):
    first_y = low(
        wide(picked(first, y)) + wide(swapped(picked(first, 1 - y), *ALONG_Y))
    )
    second_x = low(
        wide(picked(second, x, 1)) + wide(swapped(picked(second, 1 - x, 1), *ALONG_X))
    )
    first_own = low(
        wide(picked(first_y, x)) + wide(swapped(picked(first_y, 1 - x), *ALONG_X))
    )
    second_own = low(
        wide(picked(second_x, y)) + wide(swapped(picked(second_x, 1 - y), *ALONG_Y))
    )
    return first_own, second_own


def per_device_planned(
    hidden_in,
    item_ids,
    positions,
    attn_gain,
    w_query,
    key_weight,
    value_weight,
    w_output,
    ffn_gain,
    w_gate,
    w_up,
    w_down,
    out_grad,
):
    tokens, width = hidden_in.shape
    shard_rows = w_query.shape[0]
    ff = w_gate.shape[1]
    blocks = lax.axis_size("dp")
    group_ratio = QUERY_HEADS // KEY_VALUE_HEADS
    score_scale = HEAD_SIZE ** (-0.5)
    y, x, core, z_far, z_near = mesh_bits()
    quarter = z_near * 2 + core
    ff_slice = ff // blocks // 4

    gains = jnp.stack([low(attn_gain), low(ffn_gain)])
    gains = in_order(core, gains, swapped(gains, *CORE))
    gains = in_order(x, gains, swapped(gains, *ALONG_X))
    gains = in_order(y, gains, swapped(gains, *ALONG_Y))
    gains = wide(gains.reshape(blocks, 2, shard_rows).transpose(1, 0, 2).reshape(2, width))
    gain_one, gain_two = gains[0], gains[1]

    def heads_of(weight, which):
        per = weight.shape[1] // KEY_VALUE_HEADS
        split = weight.reshape(shard_rows, KEY_VALUE_HEADS // 2, 2, per)
        return low(picked(split, which, 2)).reshape(shard_rows, -1)

    def qkv_of(which):
        return jnp.concatenate(
            [heads_of(w_query, which), heads_of(key_weight, which), heads_of(value_weight, which)], 1
        )

    def both_cores(mine, for_other):
        return in_order(core, mine, swapped(for_other, *CORE))

    qkv_pair = both_cores(qkv_of(core), qkv_of(1 - core))
    q_first, q_second = gather_plane(qkv_pair[0], qkv_pair[1], y, x)
    qkv_w = jnp.stack([q_first, q_second], 2).reshape(width, -1)
    wo_shard = low(w_output).reshape(2, shard_rows // 2, width)
    o_first, o_second = gather_plane(wo_shard[0], wo_shard[1], y, x)
    output_w = jnp.stack([o_first, o_second], 2).reshape(width // 2, width)

    def columns_of(weight, which):
        split = weight.reshape(shard_rows, blocks, 4, ff_slice)
        return low(picked(split, which, 2)).reshape(shard_rows, blocks * ff_slice)

    def rows_of(weight, which):
        return low(picked(weight.reshape(4, ff_slice, width), which))

    other_quarter = z_near * 2 + 1 - core

    def ffn_weight(take, weight):
        pair = both_cores(take(weight, quarter), take(weight, other_quarter))
        first, second = gather_plane(pair[0], pair[1], y, x)
        return jnp.stack([first, second], 2).reshape(-1, pair.shape[-1])

    gate_w = ffn_weight(columns_of, w_gate)
    up_w = ffn_weight(columns_of, w_up)
    down_w = ffn_weight(rows_of, w_down)

    def with_core(block):
        return jnp.stack([block, swapped(block, *CORE)])

    def with_group(block):
        pair = jnp.stack([block, swapped(block, *Z_NEAR)])
        return jnp.concatenate([pair, swapped(pair, *CORE)], 0)

    def summed_core(parts):
        return parts[0] + swapped(parts[1], *CORE)

    def summed_group(parts):
        kept = wide(low(parts[:2])) + wide(swapped(low(parts[2:]), *CORE))
        return kept[0] + wide(swapped(low(kept[1]), *Z_NEAR))

    inputs = wide(hidden_in)
    inverse_one = lax.rsqrt(jnp.mean(inputs * inputs, -1, keepdims=True) + eps_norm)
    normed_one = inputs * inverse_one
    gained_one = with_core(low(normed_one * gain_one)).reshape(2 * tokens, width)
    marks_places = with_core(jnp.stack([item_ids + 1, positions]))
    marks = marks_places[:, 0]
    places = marks_places[:, 1].reshape(2 * tokens)
    qkv = matrix_product(gained_one, qkv_w)
    kv_heads = KEY_VALUE_HEADS // 2
    q_width = width // 2
    k_width = kv_heads * HEAD_SIZE
    query_rot = low(
        apply_rotary(qkv[:, :q_width].reshape(2 * tokens, QUERY_HEADS // 2, HEAD_SIZE), places, 1.0)
    ).reshape(2, tokens, kv_heads, group_ratio, HEAD_SIZE)
    key_rot = low(
        apply_rotary(
            qkv[:, q_width : q_width + k_width].reshape(2 * tokens, kv_heads, HEAD_SIZE), places, 1.0
        )
    ).reshape(2, tokens, k_width)
    value_low = low(qkv[:, q_width + k_width :]).reshape(2, tokens, k_width)
    key_value = jnp.concatenate([key_rot, value_low], -1)
    steps = SLIDE_SPAN // tokens
    earlier = [passed_along((key_value, marks), "seq", step) for step in range(steps, 0, -1)]
    all_kv = jnp.concatenate([e[0] for e in earlier] + [key_value], 1)
    all_marks = jnp.concatenate([e[1] for e in earlier] + [marks], 1)
    reach = SLIDE_SPAN + tokens
    all_keys = all_kv[..., :k_width].reshape(2, reach, kv_heads, HEAD_SIZE)
    all_values = all_kv[..., k_width:].reshape(2, reach, kv_heads, HEAD_SIZE)
    query_index = jnp.arange(tokens, dtype=jnp.int32)[:, None]
    key_index = jnp.arange(reach, dtype=jnp.int32)[None, :]
    distance = query_index + SLIDE_SPAN - key_index
    allowed = ((distance >= 0) & (distance <= SLIDE_SPAN))[None] & (
        marks[:, :, None] == all_marks[:, None, :]
    )

    def masked_scores():
        raw = (
            jnp.einsum("stgrd,skgd->sgrtk", query_rot, all_keys, preferred_element_type=jnp.float32)
            * score_scale
        )
        return jnp.where(allowed[:, None, None], raw, masked_fill)

    scores = masked_scores()
    row_max = jnp.max(scores, -1, keepdims=True)
    log_total = row_max + jnp.log(jnp.sum(jnp.exp(scores - row_max), -1, keepdims=True))
    probs_low = low(jnp.exp(scores - log_total))
    attended = low(
        jnp.einsum("sgrtk,skgd->stgrd", probs_low, all_values, preferred_element_type=jnp.float32)
    ).reshape(2 * tokens, q_width)
    middle = inputs + summed_core(matrix_product(attended, output_w).reshape(2, tokens, width))

    inverse_two = lax.rsqrt(jnp.mean(middle * middle, -1, keepdims=True) + eps_norm)
    normed_two = middle * inverse_two
    gained_two = with_group(low(normed_two * gain_two)).reshape(4 * tokens, width)
    out_cot = with_group(out_grad).reshape(4 * tokens, width)
    gate_pre = matrix_product(gained_two, gate_w)
    up_pre = matrix_product(gained_two, up_w)
    gate_sig = jax.nn.sigmoid(gate_pre)
    gate_act = gate_pre * gate_sig
    hidden_low = low(gate_act * up_pre)
    grad_hidden = product_transposed(out_cot, down_w)
    grad_gate_low = low(grad_hidden * up_pre * gate_sig * (1.0 + gate_pre * (1.0 - gate_sig)))
    grad_up_low = low(grad_hidden * gate_act)
    grad_gained_two = summed_group(
        (product_transposed(grad_gate_low, gate_w) + product_transposed(grad_up_low, up_w)).reshape(
            4, tokens, width
        )
    )
    layer_out = low(
        middle + summed_group(matrix_product(hidden_low, down_w).reshape(4, tokens, width))
    )
    grad_down_w = low(contract_rows(hidden_low, out_cot))
    grad_gate_w = low(contract_rows(gained_two, grad_gate_low))
    grad_up_w = low(contract_rows(gained_two, grad_up_low))

    def plane_blocks(grad):
        split = grad.reshape(2, 2, 2, -1, grad.shape[-1])
        return split[:, :, 0], split[:, :, 1]

    def for_own_rows(first, second):
        mine = chosen(core, first, second)
        return in_order(core, mine, swapped(chosen(core, second, first), *CORE))

    def ffn_shard(grad):
        rows = for_own_rows(*reduce_plane(*plane_blocks(grad), y, x))
        rows = low(wide(rows) + wide(swapped(rows, *Z_FAR)))
        return wide(in_order(z_near, rows, swapped(rows, *Z_NEAR)))

    down_shard = ffn_shard(grad_down_w).reshape(-1, width)
    gate_shard = ffn_shard(grad_gate_w)
    up_shard = ffn_shard(grad_up_w)

    def full_columns(shard):
        split = shard.reshape(4, shard_rows, blocks, ff_slice)
        return split.transpose(1, 2, 0, 3).reshape(shard_rows, ff)

    gate_shard, up_shard = full_columns(gate_shard), full_columns(up_shard)

    grad_gain_two = jnp.sum(grad_gained_two * normed_two, 0)
    grad_middle = wide(out_grad) + norm_back(grad_gained_two * gain_two, normed_two, inverse_two)

    branch = with_core(low(grad_middle)).reshape(2 * tokens, width)
    grad_output_w = low(contract_rows(attended, branch))
    grad_attended = low(product_transposed(branch, output_w)).reshape(
        2, tokens, kv_heads, group_ratio, HEAD_SIZE
    )
    probs_again = jnp.exp(masked_scores() - log_total)
    grad_probs = jnp.einsum(
        "stgrd,skgd->sgrtk", grad_attended, all_values, preferred_element_type=jnp.float32
    )
    row_dot = jnp.sum(probs_again * grad_probs, -1, keepdims=True)
    grad_scores = low(probs_again * (grad_probs - row_dot))
    grad_query = (
        jnp.einsum("sgrtk,skgd->stgrd", grad_scores, all_keys, preferred_element_type=jnp.float32)
        * score_scale
    ).reshape(2 * tokens, QUERY_HEADS // 2, HEAD_SIZE)
    grad_keys = (
        jnp.einsum("sgrtk,stgrd->skgd", grad_scores, query_rot, preferred_element_type=jnp.float32)
        * score_scale
    ).reshape(2, reach, k_width)
    grad_values = jnp.einsum(
        "sgrtk,stgrd->skgd", probs_low, grad_attended, preferred_element_type=jnp.float32
    ).reshape(2, reach, k_width)
    grad_kv = jnp.concatenate([grad_keys, grad_values], -1)
    own_kv = grad_kv[:, SLIDE_SPAN:]
    for step in range(1, steps + 1):
        first_row = SLIDE_SPAN - step * tokens
        own_kv = own_kv + wide(
            passed_along(low(grad_kv[:, first_row : first_row + tokens]), "seq", -step)
        )
    own_kv = own_kv.reshape(2 * tokens, 2 * k_width)
    grad_qkv = jnp.concatenate(
        [
            low(apply_rotary(grad_query, places, -1.0)).reshape(2 * tokens, q_width),
            low(
                apply_rotary(
                    own_kv[:, :k_width].reshape(2 * tokens, kv_heads, HEAD_SIZE), places, -1.0
                )
            ).reshape(2 * tokens, k_width),
            low(own_kv[:, k_width:]),
        ],
        1,
    )
    grad_qkv_w = low(contract_rows(gained_one, grad_qkv))
    grad_gained_one = summed_core(product_transposed(grad_qkv, qkv_w).reshape(2, tokens, width))
    grad_gain_one = jnp.sum(grad_gained_one * normed_one, 0)
    input_grad = low(grad_middle + norm_back(grad_gained_one * gain_one, normed_one, inverse_one))

    def z_sum(rows):
        halves = rows.reshape(2, rows.shape[0] // 2, rows.shape[1])
        part = low(
            wide(picked(halves, z_near)) + wide(swapped(picked(halves, 1 - z_near), *Z_NEAR))
        )
        part = low(wide(part) + wide(swapped(part, *Z_FAR)))
        return wide(in_order(z_near, part, swapped(part, *Z_NEAR))).reshape(rows.shape)

    out_blocks = grad_output_w.reshape(2, 2, 2, shard_rows // 2, width)
    out_first, out_second = reduce_plane(out_blocks[:, :, 0], out_blocks[:, :, 1], y, x)
    output_shard = z_sum(jnp.concatenate([out_first, out_second], 0))
    qkv_shard = for_own_rows(*reduce_plane(*plane_blocks(grad_qkv_w), y, x))
    qkv_shard = z_sum(qkv_shard.reshape(2 * shard_rows, -1)).reshape(2, shard_rows, -1)

    def all_heads(part):
        split = part.reshape(2, shard_rows, kv_heads, -1)
        return split.transpose(1, 2, 0, 3).reshape(shard_rows, -1)

    query_shard = all_heads(qkv_shard[..., :q_width])
    key_shard = all_heads(qkv_shard[..., q_width : q_width + k_width])
    value_shard = all_heads(qkv_shard[..., q_width + k_width :])

    gain_sums = jnp.stack([grad_gain_one, grad_gain_two])
    for hop in (CORE, ALONG_X, ALONG_Y, Z_NEAR, Z_FAR):
        gain_sums = gain_sums + swapped(gain_sums, *hop)
    mine = picked(gain_sums.reshape(2, blocks, shard_rows), lax.axis_index("dp"), 1)

    return (
        layer_out,
        input_grad,
        mine[0],
        query_shard,
        key_shard,
        value_shard,
        output_shard,
        mine[1],
        gate_shard,
        up_shard,
        down_shard,
    )


def solution(mesh):
    across, shared = P(("dp", "seq"), None), P("dp", None)
    placed = (
        across,
        P(("dp", "seq")),
        P(("dp", "seq")),
        P("dp"),
        shared,
        shared,
        shared,
        shared,
        P("dp"),
        shared,
        shared,
        shared,
        across,
    )

    def whole(*arrays):
        blocks, parts = mesh.shape["dp"], mesh.shape["seq"]
        tokens = arrays[0].shape[0] // (blocks * parts)
        planned = blocks == 8 and parts == 4 and tokens * parts == 1024
        return jax.shard_map(
            per_device_planned if planned else per_device,
            mesh=mesh,
            in_specs=placed,
            out_specs=(
                across,
                across,
                P("dp"),
                shared,
                shared,
                shared,
                shared,
                P("dp"),
                shared,
                shared,
                shared,
            ),
            check_vma=False,
        )(*arrays)

    return whole
```

```python
import functools

import jax
import jax.numpy as jnp
from jax import lax
from jax.experimental import pallas as pl
from jax.sharding import PartitionSpec as P

QUERY_HEADS = 16
KEY_VALUE_HEADS = 8
HEAD_SIZE = 96
SLIDE_SPAN = 512


eps_norm = 1e-05
rope_base = 100000.0
masked_fill = -1e30


def passed_along(block, axis, distance):
    devices = range(lax.axis_size(axis))
    route = [(i - distance, i) for i in devices if i - distance in devices]
    return lax.ppermute(block, axis, route)


def apply_rotary(value_rows, token_positions, direction):
    half_dim = value_rows.shape[-1] // 2
    frequency = rope_base ** (
        -(jnp.arange(half_dim, dtype=jnp.float32) * 2.0 / value_rows.shape[-1])
    )
    angles = token_positions.astype(jnp.float32)[:, None] * frequency[None, :]
    cosine = jnp.cos(angles)[:, None, :]
    sine_part = direction * jnp.sin(angles)[:, None, :]
    front_half = value_rows[..., :half_dim]
    back_half = value_rows[..., half_dim:]
    return jnp.concatenate(
        [front_half * cosine - back_half * sine_part, back_half * cosine + front_half * sine_part],
        -1,
    )


def matrix_product(left, right):
    return jnp.dot(left, right, preferred_element_type=jnp.float32)


def contract_rows(left, right):
    return jnp.einsum("ta,tb->ab", left, right, preferred_element_type=jnp.float32)


def product_transposed(left, right):
    return jnp.einsum("ta,ba->tb", left, right, preferred_element_type=jnp.float32)


def norm_back(grad_normed, normed, inverse):
    return inverse * (grad_normed - normed * jnp.mean(grad_normed * normed, -1, keepdims=True))


def per_device(
    hidden_in,
    item_ids,
    positions,
    attn_gain,
    w_query,
    key_weight,
    value_weight,
    w_output,
    ffn_gain,
    w_gate,
    w_up,
    w_down,
    out_grad,
):
    token_count = hidden_in.shape[0]
    query_group_count = QUERY_HEADS // KEY_VALUE_HEADS
    score_scale = HEAD_SIZE ** (-0.5)
    halo_rows = min(token_count, SLIDE_SPAN)
    halo_steps = max(1, SLIDE_SPAN // token_count)
    reduced_element_type = jnp.bfloat16
    gain_one, query_w, key_matrix, value_w, output_matrix = (
        lax.all_gather(attn_gain.astype(reduced_element_type), "dp", axis=0, tiled=True),
        lax.all_gather(w_query.astype(reduced_element_type), "dp", axis=0, tiled=True),
        lax.all_gather(key_weight.astype(reduced_element_type), "dp", axis=0, tiled=True),
        lax.all_gather(value_weight.astype(reduced_element_type), "dp", axis=0, tiled=True),
        lax.all_gather(w_output.astype(reduced_element_type), "dp", axis=0, tiled=True),
    )
    gain_two, gate_w, up_w, down_w = (
        lax.all_gather(ffn_gain.astype(reduced_element_type), "dp", axis=0, tiled=True),
        lax.all_gather(w_gate.astype(reduced_element_type), "dp", axis=0, tiled=True),
        lax.all_gather(w_up.astype(reduced_element_type), "dp", axis=0, tiled=True),
        lax.all_gather(w_down.astype(reduced_element_type), "dp", axis=0, tiled=True),
    )
    inputs = hidden_in.astype(jnp.float32)
    inverse_one = lax.rsqrt(jnp.mean(inputs * inputs, -1, keepdims=True) + eps_norm)
    normed_one = inputs * inverse_one
    gain_one_full = gain_one.astype(jnp.float32)
    scaled_first_norm = (normed_one * gain_one_full).astype(reduced_element_type)
    query_unrotated = matrix_product(scaled_first_norm, query_w).reshape(
        token_count, QUERY_HEADS, HEAD_SIZE
    )
    key_unrotated = matrix_product(scaled_first_norm, key_matrix).reshape(
        token_count, KEY_VALUE_HEADS, HEAD_SIZE
    )
    value_projected = matrix_product(scaled_first_norm, value_w)
    query_rot = (
        apply_rotary(query_unrotated, positions, 1.0)
        .astype(reduced_element_type)
        .reshape(token_count, KEY_VALUE_HEADS, query_group_count, HEAD_SIZE)
    )
    key_rot = apply_rotary(key_unrotated, positions, 1.0).astype(reduced_element_type)
    value_reduced = value_projected.astype(reduced_element_type).reshape(
        token_count, KEY_VALUE_HEADS, HEAD_SIZE
    )
    item_marks = item_ids + 1
    key_parts = []
    value_parts = []
    mark_parts = []
    for offset in range(halo_steps, 0, -1):
        incoming = passed_along((key_rot, value_reduced, item_marks), ("dp", "seq"), offset)
        key_parts.append(incoming[0])
        value_parts.append(incoming[1])
        mark_parts.append(incoming[2])
    all_keys = jnp.concatenate(key_parts + [key_rot], 0)
    all_values = jnp.concatenate(value_parts + [value_reduced], 0)
    all_marks = jnp.concatenate(mark_parts + [item_marks], 0)
    query_index = jnp.arange(token_count, dtype=jnp.int32)[:, None]
    key_index = jnp.arange(SLIDE_SPAN + token_count, dtype=jnp.int32)[None, :]
    distance = query_index + SLIDE_SPAN - key_index
    allowed = (
        (distance >= 0) & (distance <= SLIDE_SPAN) & (item_marks[:, None] == all_marks[None, :])
    )

    def masked_scores():
        raw_scores = (
            jnp.einsum("tgrd,kgd->grtk", query_rot, all_keys, preferred_element_type=jnp.float32)
            * score_scale
        )
        return jnp.where(allowed[None, None], raw_scores, masked_fill)

    scores = masked_scores()
    row_max = jnp.max(scores, -1, keepdims=True)
    log_total = row_max + jnp.log(jnp.sum(jnp.exp(scores - row_max), -1, keepdims=True))
    probs_low = jnp.exp(scores - log_total).astype(reduced_element_type)
    attended_low = (
        jnp.einsum("grtk,kgd->tgrd", probs_low, all_values, preferred_element_type=jnp.float32)
        .reshape(token_count, QUERY_HEADS * HEAD_SIZE)
        .astype(reduced_element_type)
    )
    middle = inputs + matrix_product(attended_low, output_matrix)
    inverse_two = lax.rsqrt(jnp.mean(middle * middle, -1, keepdims=True) + eps_norm)
    normed_two = middle * inverse_two
    gain_two_full = gain_two.astype(jnp.float32)
    gained_two = (normed_two * gain_two_full).astype(reduced_element_type)
    gate_pre = matrix_product(gained_two, gate_w)
    up_pre = matrix_product(gained_two, up_w)
    gate_sig = jax.nn.sigmoid(gate_pre)
    gate_act = gate_pre * gate_sig
    hidden_low = (gate_act * up_pre).astype(reduced_element_type)
    layer_out = (middle + matrix_product(hidden_low, down_w)).astype(reduced_element_type)
    grad_down_w = contract_rows(hidden_low, out_grad)
    grad_hidden = product_transposed(out_grad, down_w)
    grad_gate_low = (grad_hidden * up_pre * gate_sig * (1.0 + gate_pre * (1.0 - gate_sig))).astype(
        reduced_element_type
    )
    grad_up_low = (grad_hidden * gate_act).astype(reduced_element_type)
    grad_gate_w = contract_rows(gained_two, grad_gate_low)
    grad_up_w = contract_rows(gained_two, grad_up_low)
    grad_gained_two = product_transposed(grad_gate_low, gate_w) + product_transposed(
        grad_up_low, up_w
    )
    grad_gain_two = jnp.sum(grad_gained_two * normed_two, 0)
    grad_middle = out_grad.astype(jnp.float32) + norm_back(
        grad_gained_two * gain_two_full, normed_two, inverse_two
    )
    ffn_shards = (
        lax.psum_scatter(grad_gain_two, "dp", scatter_dimension=0, tiled=True),
        lax.psum_scatter(grad_gate_w, "dp", scatter_dimension=0, tiled=True),
        lax.psum_scatter(grad_up_w, "dp", scatter_dimension=0, tiled=True),
        lax.psum_scatter(grad_down_w, "dp", scatter_dimension=0, tiled=True),
    )
    branch_gradient = grad_middle.astype(reduced_element_type)
    grad_output_w = contract_rows(attended_low, branch_gradient)
    grad_attended = (
        product_transposed(branch_gradient, output_matrix)
        .astype(reduced_element_type)
        .reshape(token_count, KEY_VALUE_HEADS, query_group_count, HEAD_SIZE)
    )
    scores_again = masked_scores()
    probs_again = jnp.exp(scores_again - log_total)
    grad_probs = jnp.einsum(
        "tgrd,kgd->grtk", grad_attended, all_values, preferred_element_type=jnp.float32
    )
    row_dot = jnp.sum(probs_again * grad_probs, -1, keepdims=True)
    grad_scores = (probs_again * (grad_probs - row_dot)).astype(reduced_element_type)
    grad_query = (
        jnp.einsum(
            "grtk,kgd->tgrd", grad_scores, all_keys, preferred_element_type=jnp.float32
        ).reshape(token_count, QUERY_HEADS, HEAD_SIZE)
        * score_scale
    )
    grad_keys = (
        jnp.einsum("grtk,tgrd->kgd", grad_scores, query_rot, preferred_element_type=jnp.float32)
        * score_scale
    )
    grad_values = jnp.einsum(
        "grtk,tgrd->kgd", probs_low, grad_attended, preferred_element_type=jnp.float32
    )
    key_neighbourhood = grad_keys[SLIDE_SPAN:]
    value_neighbourhood = grad_values[SLIDE_SPAN:]
    for offset in range(1, halo_steps + 1):
        first_row = (halo_steps - offset) * halo_rows
        returned = passed_along(
            (
                grad_keys[first_row : first_row + halo_rows],
                grad_values[first_row : first_row + halo_rows],
            ),
            ("dp", "seq"),
            -offset,
        )
        key_neighbourhood = key_neighbourhood.at[token_count - halo_rows :].add(returned[0])
        value_neighbourhood = value_neighbourhood.at[token_count - halo_rows :].add(returned[1])
    grad_query_low = (
        apply_rotary(grad_query, positions, -1.0)
        .astype(reduced_element_type)
        .reshape(token_count, QUERY_HEADS * HEAD_SIZE)
    )
    key_gradient_reduced = (
        apply_rotary(key_neighbourhood, positions, -1.0)
        .astype(reduced_element_type)
        .reshape(token_count, KEY_VALUE_HEADS * HEAD_SIZE)
    )
    value_gradient_reduced = value_neighbourhood.astype(reduced_element_type).reshape(
        token_count, KEY_VALUE_HEADS * HEAD_SIZE
    )
    grad_query_w = contract_rows(scaled_first_norm, grad_query_low)
    grad_key_w = contract_rows(scaled_first_norm, key_gradient_reduced)
    grad_value_w = contract_rows(scaled_first_norm, value_gradient_reduced)
    grad_gained_one = (
        product_transposed(grad_query_low, query_w)
        + product_transposed(key_gradient_reduced, key_matrix)
        + product_transposed(value_gradient_reduced, value_w)
    )
    grad_gain_one = jnp.sum(grad_gained_one * normed_one, 0)
    input_grad = (
        grad_middle + norm_back(grad_gained_one * gain_one_full, normed_one, inverse_one)
    ).astype(reduced_element_type)
    attn_shards = (
        lax.psum_scatter(grad_gain_one, "dp", scatter_dimension=0, tiled=True),
        lax.psum_scatter(grad_query_w, "dp", scatter_dimension=0, tiled=True),
        lax.psum_scatter(grad_key_w, "dp", scatter_dimension=0, tiled=True),
        lax.psum_scatter(grad_value_w, "dp", scatter_dimension=0, tiled=True),
        lax.psum_scatter(grad_output_w, "dp", scatter_dimension=0, tiled=True),
    )
    summed = lax.psum(
        (
            attn_shards[0],
            attn_shards[1],
            attn_shards[2],
            attn_shards[3],
            attn_shards[4],
            ffn_shards[0],
            ffn_shards[1],
            ffn_shards[2],
            ffn_shards[3],
        ),
        "seq",
    )
    return (
        layer_out,
        input_grad,
        summed[0],
        summed[1],
        summed[2],
        summed[3],
        summed[4],
        summed[5],
        summed[6],
        summed[7],
        summed[8],
    )


CORE, ALONG_X, ALONG_Y = ("dp", 1), ("dp", 2), ("dp", 4)
Z_NEAR, Z_FAR = ("seq", 1), ("seq", 2)
QUERY_TILE = 256


def swapped(block, hop):
    axis, bit = hop
    route = [(i, i ^ bit) for i in range(lax.axis_size(axis))]
    return lax.ppermute(block, axis, route)


def chosen(bit, first, second):
    return jnp.where(bit == 0, first, second)


def in_order(bit, own, other):
    return chosen(bit, jnp.stack([own, other]), jnp.stack([other, own]))


def picked(blocks, index, axis=0):
    return lax.dynamic_index_in_dim(blocks, index, axis, keepdims=False)


def wide(v):
    return v.astype(jnp.float32)


def low(v):
    return v.astype(jnp.bfloat16)


def gather_plane(first, second, y, x):
    first_x = in_order(x, first, swapped(first, ALONG_X))
    second_y = in_order(y, second, swapped(second, ALONG_Y))
    first_all = in_order(y, first_x, swapped(first_x, ALONG_Y))
    second_other = swapped(second_y, ALONG_X)
    second_all = chosen(
        x,
        jnp.stack([second_y, second_other], 1),
        jnp.stack([second_other, second_y], 1),
    )
    return first_all, second_all


def reduce_plane(first, second, y, x):
    first_y = low(wide(picked(first, y)) + wide(swapped(picked(first, 1 - y), ALONG_Y)))
    second_x = low(wide(picked(second, x, 1)) + wide(swapped(picked(second, 1 - x, 1), ALONG_X)))
    first_own = low(wide(picked(first_y, x)) + wide(swapped(picked(first_y, 1 - x), ALONG_X)))
    second_own = low(wide(picked(second_x, y)) + wide(swapped(picked(second_x, 1 - y), ALONG_Y)))
    return first_own, second_own


def tile_mask(marks_q, marks_k):
    shape = (QUERY_TILE, marks_k.shape[-1])
    distance = (
        lax.broadcasted_iota(jnp.int32, shape, 0)
        + SLIDE_SPAN
        - lax.broadcasted_iota(jnp.int32, shape, 1)
    )
    return (distance >= 0) & (distance <= SLIDE_SPAN) & (marks_q == marks_k)


def head_columns(block, index):
    return block[:, index * HEAD_SIZE : (index + 1) * HEAD_SIZE]


def attention_tile(q_ref, kv_ref, marks_q_ref, marks_k_ref):
    reach = SLIDE_SPAN + QUERY_TILE
    start = pl.multiple_of(pl.program_id(1) * QUERY_TILE, QUERY_TILE)
    window = pl.ds(start, reach)
    allowed = tile_mask(marks_q_ref[0], marks_k_ref[0, :, window])
    return window, allowed, q_ref[0], kv_ref[0, window, :]


def nt_product(left, right):
    return lax.dot_general(
        left, right, (((1,), (1,)), ((), ())), preferred_element_type=jnp.float32
    )


def tn_product(left, right):
    return lax.dot_general(
        left, right, (((0,), (0,)), ((), ())), preferred_element_type=jnp.float32
    )


def attention_forward_kernel(heads, q_ref, kv_ref, marks_q_ref, marks_k_ref, out_ref, lse_ref):
    _, allowed, queries, pairs = attention_tile(q_ref, kv_ref, marks_q_ref, marks_k_ref)
    scale = HEAD_SIZE ** (-0.5)
    outs, sums = [], []
    for head in range(heads):
        keys = head_columns(pairs, head // 2)
        values = head_columns(pairs, heads // 2 + head // 2)
        scores = jnp.where(
            allowed, nt_product(head_columns(queries, head), keys) * scale, masked_fill
        )
        top = jnp.max(scores, -1, keepdims=True)
        total = top + jnp.log(jnp.sum(jnp.exp(scores - top), -1, keepdims=True))
        probs = jnp.exp(scores - total).astype(jnp.bfloat16)
        outs.append(jnp.dot(probs, values, preferred_element_type=jnp.float32))
        sums.append(total)
    out_ref[0] = jnp.concatenate(outs, 1).astype(jnp.bfloat16)
    lse_ref[0] = jnp.concatenate(sums, 1)


def attention_backward_kernel(
    heads, q_ref, kv_ref, marks_q_ref, marks_k_ref, lse_ref, do_ref, dq_ref, dkv_ref
):
    window, allowed, queries, pairs = attention_tile(q_ref, kv_ref, marks_q_ref, marks_k_ref)
    scale = HEAD_SIZE ** (-0.5)

    @pl.when(pl.program_id(1) == 0)
    def _():
        dkv_ref[...] = jnp.zeros_like(dkv_ref)

    outer, sums = do_ref[0], lse_ref[0]
    dqs, dks, dvs = [], [], []
    for head in range(heads):
        keys = head_columns(pairs, head // 2)
        values = head_columns(pairs, heads // 2 + head // 2)
        query, grad = head_columns(queries, head), head_columns(outer, head)
        scores = jnp.where(allowed, nt_product(query, keys) * scale, masked_fill)
        probs = jnp.exp(scores - sums[:, head : head + 1])
        grad_probs = nt_product(grad, values)
        row_dot = jnp.sum(probs * grad_probs, -1, keepdims=True)
        grad_scores = (probs * (grad_probs - row_dot)).astype(jnp.bfloat16)
        dqs.append(jnp.dot(grad_scores, keys, preferred_element_type=jnp.float32) * scale)
        dk = tn_product(grad_scores, query) * scale
        dv = tn_product(probs.astype(jnp.bfloat16), grad)
        if head % 2 == 0:
            dks.append(dk)
            dvs.append(dv)
        else:
            dks[-1] += dk
            dvs[-1] += dv
    dq_ref[0] = jnp.concatenate(dqs, 1)
    dkv_ref[0, window, :] += jnp.concatenate(dks + dvs, 1)


def attention_specs(heads, reach):
    width = heads * HEAD_SIZE
    tile = pl.BlockSpec((1, QUERY_TILE, width), lambda s, i: (s, i, 0))
    return (
        (
            tile,
            pl.BlockSpec((1, reach, width), lambda s, i: (s, 0, 0)),
            pl.BlockSpec((1, QUERY_TILE, 1), lambda s, i: (s, i, 0)),
            pl.BlockSpec((1, 1, reach), lambda s, i: (s, 0, 0)),
        ),
        pl.BlockSpec((1, QUERY_TILE, heads), lambda s, i: (s, i, 0)),
        tile,
        pl.BlockSpec((1, reach, width), lambda s, i: (s, 0, 0)),
    )


def attention_cost(queries, heads, products):
    pairs = queries.shape[0] * queries.shape[1] * (SLIDE_SPAN + QUERY_TILE) * heads
    return pl.CostEstimate(
        flops=2 * pairs * HEAD_SIZE * products, transcendentals=pairs * 2, bytes_accessed=1 << 22
    )


def attention_forward(queries, pairs, marks_q, marks_k):
    sequences, tokens, width = queries.shape
    heads = width // HEAD_SIZE
    inputs, sums, tile, _ = attention_specs(heads, pairs.shape[1])
    return pl.pallas_call(
        functools.partial(attention_forward_kernel, heads),
        grid=(sequences, tokens // QUERY_TILE),
        in_specs=inputs,
        out_specs=(tile, sums),
        out_shape=(
            jax.ShapeDtypeStruct(queries.shape, jnp.bfloat16),
            jax.ShapeDtypeStruct((sequences, tokens, heads), jnp.float32),
        ),
        cost_estimate=attention_cost(queries, heads, 2),
        name="attention_forward",
    )(queries, pairs, marks_q, marks_k)


def attention_backward(queries, pairs, marks_q, marks_k, lse, outer):
    sequences, tokens, width = queries.shape
    heads = width // HEAD_SIZE
    inputs, sums, tile, whole = attention_specs(heads, pairs.shape[1])
    return pl.pallas_call(
        functools.partial(attention_backward_kernel, heads),
        grid=(sequences, tokens // QUERY_TILE),
        in_specs=inputs + (sums, tile),
        out_specs=(tile, whole),
        out_shape=(
            jax.ShapeDtypeStruct(queries.shape, jnp.float32),
            jax.ShapeDtypeStruct(pairs.shape, jnp.float32),
        ),
        cost_estimate=attention_cost(queries, heads, 5),
        name="attention_backward",
    )(queries, pairs, marks_q, marks_k, lse, outer)


def half_swapped(rows):
    half = HEAD_SIZE // 2
    lane = lax.broadcasted_iota(jnp.int32, rows.shape, 1) % HEAD_SIZE
    return jnp.where(lane < half, jnp.roll(rows, -half, 1), jnp.roll(rows, half, 1))


def per_device_planned(*arrays):
    return planned_step(*arrays)


def planned_step(
    hidden_in,
    item_ids,
    positions,
    attn_gain,
    w_query,
    key_weight,
    value_weight,
    w_output,
    ffn_gain,
    w_gate,
    w_up,
    w_down,
    out_grad,
):
    tokens, width = hidden_in.shape
    shard_rows = w_query.shape[0]
    ff = w_gate.shape[1]
    blocks = lax.axis_size("dp")
    block, part = lax.axis_index("dp"), lax.axis_index("seq")
    y, x, core = block // 4, (block // 2) % 2, block % 2
    z_near = part % 2
    quarter = z_near * 2 + core
    other_quarter = z_near * 2 + 1 - core
    ff_slice = ff // blocks // 4
    pair_tokens = 2 * tokens
    kv_heads = KEY_VALUE_HEADS // 4
    k_width = kv_heads * HEAD_SIZE
    q_width = width // 4
    rope_width = q_width + k_width

    def for_cores(take):
        mine = chosen(core, take(0), take(1))
        return mine, chosen(core, take(1), take(0))

    def qkv_of(core_bit):
        def heads_of(weight, x_bit):
            per = weight.shape[1] // KEY_VALUE_HEADS
            near, far = 2 * x_bit + core_bit, 4 + 2 * x_bit + core_bit
            return low(
                chosen(
                    z_near, weight[:, near * per : (near + 1) * per], weight[:, far * per : (far + 1) * per]
                )
            )

        return jnp.concatenate(
            [heads_of(w, b) for w in (w_query, key_weight, value_weight) for b in (0, 1)], 1
        )

    def columns_of(weight):
        def take(core_bit):
            def piece(d, which):
                start = (d * 4 + which) * ff_slice
                return weight[:, start : start + ff_slice]

            return jnp.concatenate(
                [
                    low(chosen(z_near, piece(d, core_bit), piece(d, 2 + core_bit)))
                    for d in range(blocks)
                ],
                1,
            )

        return for_cores(take)

    def rows_of(weight):
        split = weight.reshape(4, ff_slice, width)
        return low(picked(split, quarter)), low(picked(split, other_quarter))

    def gathered(mine_other):
        mine, for_other = mine_other
        pair = in_order(core, mine, swapped(for_other, CORE))
        first, second = gather_plane(pair[0], pair[1], y, x)
        return jnp.stack([first, second], 2).reshape(-1, mine.shape[-1])

    gains = jnp.stack([low(attn_gain), low(ffn_gain)])
    gains = in_order(core, gains, swapped(gains, CORE))
    gains = in_order(x, gains, swapped(gains, ALONG_X))
    gains = in_order(y, gains, swapped(gains, ALONG_Y))
    gains = wide(gains.reshape(blocks, 2, shard_rows).transpose(1, 0, 2).reshape(2, width))
    gain_one, gain_two = gains[0], gains[1]

    qkv_w = gathered(for_cores(qkv_of))
    wo_shard = low(w_output).reshape(2, shard_rows // 2, width)
    o_first, o_second = gather_plane(wo_shard[0], wo_shard[1], y, x)
    output_w = jnp.stack([o_first, o_second], 2).reshape(width // 2, width)
    gate_w = gathered(columns_of(w_gate))
    up_w = gathered(columns_of(w_up))
    down_w = gathered(rows_of(w_down))

    def with_group(rows):
        pair = in_order(z_near, rows, swapped(rows, Z_NEAR))
        return jnp.stack([pair, swapped(pair, CORE)]).reshape(4 * tokens, -1)

    def summed_group(parts):
        parts = parts.reshape(2, 2, tokens, width)
        kept = wide(low(parts[0])) + wide(swapped(low(parts[1]), CORE))
        return picked(kept, z_near) + wide(swapped(low(picked(kept, 1 - z_near)), Z_NEAR))

    facts = jnp.stack([item_ids + 1, positions])
    facts = in_order(z_near, facts, swapped(facts, Z_NEAR))
    facts = jnp.stack([facts, swapped(facts, CORE)])
    marks = facts[:, :, 0].reshape(2, pair_tokens)
    places = facts[:, :, 1].reshape(4 * tokens)
    half = HEAD_SIZE // 2
    frequency = rope_base ** (-(jnp.arange(half, dtype=jnp.float32) * 2.0 / HEAD_SIZE))
    angles = wide(places)[:, None] * frequency[None, :]
    cosine, sine = lax.optimization_barrier((jnp.cos(angles), jnp.sin(angles)))
    heads = rope_width // HEAD_SIZE
    cosine, sine = lax.optimization_barrier(
        (jnp.concatenate([cosine] * 2 * heads, 1), jnp.concatenate([-sine, sine] * heads, 1))
    )

    inputs = wide(hidden_in)
    inverse_one = lax.rsqrt(jnp.mean(inputs * inputs, -1, keepdims=True) + eps_norm)
    normed_one = inputs * inverse_one
    gained_one = with_group(low(normed_one * gain_one))
    qkv = matrix_product(gained_one, qkv_w)
    turned = low(qkv[:, :rope_width] * cosine + half_swapped(qkv[:, :rope_width]) * sine)
    query_rot = turned[:, :q_width].reshape(2, pair_tokens, q_width)
    key_value = jnp.concatenate([turned[:, q_width:], low(qkv[:, rope_width:])], 1).reshape(
        2, pair_tokens, 2 * k_width
    )

    def passed(rows, step):
        return passed_along(rows, "seq", step)

    steps = SLIDE_SPAN // tokens
    all_kv = jnp.concatenate([passed(key_value, steps), key_value], 1)
    all_marks = jnp.concatenate([passed(marks, steps), marks], 1)
    marks_q, marks_k = marks[:, :, None], all_marks[:, None, :]
    attended, log_total = attention_forward(query_rot, all_kv, marks_q, marks_k)

    def between_heads_and_tokens(rows):
        other = swapped(picked(rows, 1 - z_near, 1), Z_NEAR)
        own = picked(rows, z_near, 1)
        return chosen(
            z_near, jnp.concatenate([own, other], -1), jnp.concatenate([other, own], -1)
        )

    attended = between_heads_and_tokens(attended.reshape(2, 2, tokens, q_width)).reshape(
        2 * tokens, 2 * q_width
    )
    partial = matrix_product(attended, output_w).reshape(2, tokens, width)
    middle = inputs + partial[0] + swapped(partial[1], CORE)

    inverse_two = lax.rsqrt(jnp.mean(middle * middle, -1, keepdims=True) + eps_norm)
    normed_two = middle * inverse_two
    gained_two = with_group(low(normed_two * gain_two))
    out_cot = with_group(out_grad)
    gate_pre = matrix_product(gained_two, gate_w)
    up_pre = matrix_product(gained_two, up_w)
    gate_sig = jax.nn.sigmoid(gate_pre)
    gate_act = gate_pre * gate_sig
    hidden_low = low(gate_act * up_pre)
    grad_hidden = product_transposed(out_cot, down_w)
    grad_gate_low = low(grad_hidden * up_pre * gate_sig * (1.0 + gate_pre * (1.0 - gate_sig)))
    grad_up_low = low(grad_hidden * gate_act)
    partial_two = product_transposed(grad_gate_low, gate_w) + product_transposed(grad_up_low, up_w)
    grad_gained_two = summed_group(partial_two)

    gained_late, gate_late, up_late, hidden_late, _ = lax.optimization_barrier(
        (gained_two, grad_gate_low, grad_up_low, hidden_low, partial_two)
    )
    grad_down_w = low(contract_rows(hidden_late, out_cot))
    grad_gate_w = low(contract_rows(gained_late, gate_late))
    grad_up_w = low(contract_rows(gained_late, up_late))
    layer_out = low(middle + summed_group(matrix_product(hidden_late, down_w)))

    def own_shard(grad):
        split = grad.reshape(2, 2, 2, -1, grad.shape[-1])
        first, second = reduce_plane(split[:, :, 0], split[:, :, 1], y, x)
        mine = chosen(core, first, second)
        rows = in_order(core, mine, swapped(chosen(core, second, first), CORE))
        rows = low(wide(rows) + wide(swapped(rows, Z_FAR)))
        other = swapped(rows, Z_NEAR)
        return [
            chosen(z_near, one, two)[bit] for one, two in ((rows, other), (other, rows)) for bit in (0, 1)
        ]

    def full_columns(quarters):
        return wide(
            jnp.concatenate(
                [
                    quarters[q][:, d * ff_slice : (d + 1) * ff_slice]
                    for d in range(blocks)
                    for q in range(4)
                ],
                1,
            )
        )

    down_shard = wide(jnp.concatenate(own_shard(grad_down_w), 0))
    gate_shard = full_columns(own_shard(grad_gate_w))
    up_shard = full_columns(own_shard(grad_up_w))

    grad_gain_two = jnp.sum(grad_gained_two * normed_two, 0)
    grad_middle = wide(out_grad) + norm_back(grad_gained_two * gain_two, normed_two, inverse_two)

    branch = low(grad_middle)
    branch = jnp.stack([branch, swapped(branch, CORE)]).reshape(2 * tokens, width)
    grad_attended = low(product_transposed(branch, output_w)).reshape(2, tokens, 2, q_width)
    other_outer = swapped(picked(grad_attended, 1 - z_near, 2), Z_NEAR)
    own_outer = picked(grad_attended, z_near, 2)
    outer = chosen(
        z_near,
        jnp.concatenate([own_outer, other_outer], 1),
        jnp.concatenate([other_outer, own_outer], 1),
    )
    grad_query, grad_kv = attention_backward(
        query_rot, all_kv, marks_q, marks_k, log_total, outer
    )
    own_kv = grad_kv[:, SLIDE_SPAN:] + wide(passed(low(grad_kv[:, :SLIDE_SPAN]), -steps))
    grad_turned = jnp.concatenate([grad_query, own_kv[..., :k_width]], -1).reshape(
        4 * tokens, rope_width
    )
    grad_qkv = jnp.concatenate(
        [
            low(grad_turned * cosine - half_swapped(grad_turned) * sine),
            low(own_kv[..., k_width:].reshape(4 * tokens, k_width)),
        ],
        1,
    )
    grad_qkv_w = low(contract_rows(gained_one, grad_qkv))
    grad_gained_one = summed_group(product_transposed(grad_qkv, qkv_w))
    grad_gain_one = jnp.sum(grad_gained_one * normed_one, 0)
    input_grad = low(grad_middle + norm_back(grad_gained_one * gain_one, normed_one, inverse_one))

    grad_output_w = low(contract_rows(attended, branch))
    out_blocks = grad_output_w.reshape(2, 2, 2, shard_rows // 2, width)
    out_first, out_second = reduce_plane(out_blocks[:, :, 0], out_blocks[:, :, 1], y, x)
    mine = chosen(z_near, out_first, out_second)
    mine = low(wide(mine) + wide(swapped(chosen(z_near, out_second, out_first), Z_NEAR)))
    mine = low(wide(mine) + wide(swapped(mine, Z_FAR)))
    output_shard = wide(in_order(z_near, mine, swapped(mine, Z_NEAR))).reshape(shard_rows, width)
    qkv_quarters = own_shard(grad_qkv_w)

    def all_heads(start, per):
        return wide(
            jnp.concatenate(
                [
                    qkv_quarters[2 * zn + c][:, start + xb * per : start + (xb + 1) * per]
                    for zn in (0, 1)
                    for xb in (0, 1)
                    for c in (0, 1)
                ],
                1,
            )
        )

    query_shard = all_heads(0, q_width // 2)
    key_shard = all_heads(q_width, k_width // 2)
    value_shard = all_heads(rope_width, k_width // 2)

    def gain_shard(grad):
        halves = (CORE, ALONG_X, ALONG_Y, Z_NEAR, Z_FAR)
        for hop in halves:
            grad = grad + swapped(grad, hop)
        return picked(grad.reshape(blocks, shard_rows), block)

    return (
        layer_out,
        input_grad,
        gain_shard(grad_gain_one),
        query_shard,
        key_shard,
        value_shard,
        output_shard,
        gain_shard(grad_gain_two),
        gate_shard,
        up_shard,
        down_shard,
    )


def solution(mesh):
    across, shared = P(("dp", "seq"), None), P("dp", None)
    placed = (
        across,
        P(("dp", "seq")),
        P(("dp", "seq")),
        P("dp"),
        shared,
        shared,
        shared,
        shared,
        P("dp"),
        shared,
        shared,
        shared,
        across,
    )

    def whole(*arrays):
        blocks, parts = mesh.shape["dp"], mesh.shape["seq"]
        tokens = arrays[0].shape[0] // (blocks * parts)
        planned = blocks == 8 and parts == 4 and tokens * parts == 1024
        step = jax.shard_map(
            per_device_planned if planned else per_device,
            mesh=mesh,
            in_specs=placed,
            out_specs=(
                across,
                across,
                P("dp"),
                shared,
                shared,
                shared,
                shared,
                P("dp"),
                shared,
                shared,
                shared,
            ),
            check_vma=False,
        )
        return step(*arrays)

    return whole
```
